512 devices in a mesh: replica: 32 (over z_hi, y, core), fsdp: 16 (over x, z_lo).
Axes of the slice: x: 4, y: 8, z: 8 (z_hi: 2, z_lo: 4; z = z_hi * 4 + z_lo), core: 2. Of those that a mesh axis runs over, the one named last changes fastest.
Arguments:
- hidden_states: bfloat16 [32, 4096, 4096], P('replica', 'fsdp'), may hold values from -6 to 6
- norm_gain: bfloat16 [32, 4096], P('replica', 'fsdp'), may hold values from 0.5 to 1.5
- key_weight: bfloat16 [32, 4096, 1024], P('replica', 'fsdp'), may hold values from -0.09375 to 0.09375
- value_weight: bfloat16 [32, 4096, 1024], P('replica', 'fsdp'), may hold values from -0.09375 to 0.09375
- deltas: float32 [32, 256, 4096], P('replica', 'fsdp'), may hold values from -6 to 6
- outer_params: float32 [256, 4096], P('fsdp', 'replica'), may hold values from -6 to 6
- momentum: float32 [256, 4096], P('fsdp', 'replica'), may hold values from -3 to 3
- local_params: bfloat16 [32, 256, 4096], P('replica', 'fsdp'), may hold values from -6 to 6
Outputs:
- keys: bfloat16 [32, 4096, 1024], P('replica', 'fsdp')
- values: bfloat16 [32, 4096, 1024], P('replica', 'fsdp')
- momentum_new: float32 [256, 4096], P('fsdp', 'replica')
- outer_new: float32 [256, 4096], P('fsdp', 'replica')
- local_new: bfloat16 [32, 256, 4096], P('replica', 'fsdp')
The draws below stay inside these ranges and needn't reach their ends.
All inputs are finite; a program needn't handle non-finite values.
Results may differ from the reference program's by a relative error of at most 0.0085.
Values may be sent and summed in bfloat16 or wider, within the bound.
No kernel may reach another device: no remote copies, remote signals or barrier semaphores. Data moves between devices by JAX's collectives and lax.ppermute only.
A program may use at most 128 MiB of HBM per device.

```python
import jax
import jax.numpy as jnp
from jax import lax

D = 4096
HEAD = 128
KV = 1024
TOK_DEV = 256
TOKENS_R = 4096
FRAG_ROWS = 256
N_REPLICA = 32


def raised(entries, key, source, target, parts, factor):
    def block_of(axis_at):
        return (jnp.arange(entries.shape[axis_at]) // (entries.shape[axis_at] // parts)).reshape((-1,) + (1,) * (entries.ndim - 1 - axis_at))

    one_side = jax.random.permutation(key, parts)[block_of(target)]
    second = (block_of(target) + parts // 2) % parts
    return jnp.where((block_of(source) == one_side) | (block_of(source) == second), factor * entries, entries)


def levels(rng, extent, pieces, smallest, high):
    loudness = 1.0
    for position, shards_of in pieces:
        draws = jax.random.uniform(jax.random.fold_in(jax.random.fold_in(rng, 6), position), (shards_of,), jnp.float32, smallest / len(pieces), high / len(pieces))
        loudness = loudness * jnp.repeat(jnp.exp(draws), extent[position] // shards_of).reshape((-1,) + (1,) * (len(extent) - 1 - position))
    return loudness


def bell_draw(key, dims, deviation, reach, shards=(), held_as=jnp.bfloat16):
    values = deviation * jax.random.normal(key, dims, jnp.float32)
    if shards:
        values = values * levels(key, dims, shards, -0.22, 0.18)
    return jnp.clip(values, -reach, reach).astype(held_as)


def heavy_noise(stream_key, shape, scale, most, shards, heavy, kind=jnp.bfloat16):
    result = scale * jax.random.normal(stream_key, shape, jnp.float32)
    if shards:
        result = result * levels(stream_key, shape, shards, -0.22, 0.18)
    return jnp.clip(raised(result, jax.random.fold_in(stream_key, 3), *heavy), -most, most).astype(kind)


def setup_inputs(seed: int = 0) -> dict:
    key_list = jax.random.split(jax.random.key(seed), 9)
    return {
        "hidden_states": bell_draw(key_list[0], (N_REPLICA, TOKENS_R, D), 1.0, 6.0, ((0, 32), (1, 16))),
        "norm_gain": jnp.clip(1.0 + 0.1 * jax.random.normal(key_list[1], (N_REPLICA, D), jnp.float32), 0.5, 1.5).astype(jnp.bfloat16),
        "key_weight": bell_draw(key_list[2], (N_REPLICA, D, KV), D ** -0.5, 0.09375, ((0, 32), (1, 16))),
        "value_weight": bell_draw(key_list[3], (N_REPLICA, D, KV), D ** -0.5, 0.09375, ((0, 32), (1, 16))),
        "deltas": heavy_noise(key_list[4], (N_REPLICA, FRAG_ROWS, D), 1.0, 6.0, ((0, 32), (1, 16)), (0, 2, 32, 2.75), jnp.float32),
        "outer_params": bell_draw(key_list[5], (FRAG_ROWS, D), 1.0, 6.0, ((0, 16), (1, 32)), jnp.float32),
        "momentum": bell_draw(key_list[6], (FRAG_ROWS, D), 0.5, 3.0, ((0, 16), (1, 32)), jnp.float32),
        "local_params": bell_draw(key_list[7], (N_REPLICA, FRAG_ROWS, D), 1.0, 6.0, ((0, 32), (1, 16))),
    }


def rotate_keys(keys_raw, positions, head_size):
    half_width = head_size // 2
    exponent = jnp.arange(half_width, dtype=jnp.float32) * (2.0 / head_size)
    frequency = jnp.power(jnp.float32(500000.0), -exponent)
    angles = positions.astype(jnp.float32)[:, None] * frequency[None, :]
    cosine_table = jnp.cos(angles)[:, None, :]
    sine_table = jnp.sin(angles)[:, None, :]
    shaped = keys_raw.reshape(keys_raw.shape[0], -1, head_size)
    first_half = shaped[:, :, :half_width]
    second_half = shaped[:, :, half_width:]
    turned = jnp.concatenate([first_half * cosine_table - second_half * sine_table, second_half * cosine_table + first_half * sine_table], axis=2)
    return turned.reshape(keys_raw.shape)

def project_replica(inputs):
    states, gain, weight_key, weight_value = inputs
    states32 = states.astype(jnp.float32)
    inv_rms = lax.rsqrt(lax.optimization_barrier(jnp.mean(states32 * states32, axis=1, keepdims=True)) + 1e-05)
    normed = (states32 * inv_rms * gain.astype(jnp.float32)[None, :]).astype(jnp.bfloat16)
    keys_raw = jnp.dot(normed, weight_key, preferred_element_type=jnp.float32)
    values_raw = jnp.dot(normed, weight_value, preferred_element_type=jnp.float32)
    positions = jnp.arange(states.shape[0], dtype=jnp.int32) % TOK_DEV
    rotated = rotate_keys(keys_raw, positions, HEAD)
    return (rotated.astype(jnp.bfloat16), values_raw.astype(jnp.bfloat16))

def reference(hidden_states, norm_gain, key_weight, value_weight, deltas, outer_params, momentum, local_params):
    keys, values = lax.map(project_replica, (hidden_states, norm_gain, key_weight, value_weight))
    avg_delta = lax.optimization_barrier(jnp.sum(deltas, axis=0)) / deltas.shape[0]
    momentum_new = 0.9 * momentum + avg_delta
    outer_new = outer_params - 0.7 * (avg_delta + 0.9 * momentum_new)
    local_new = (0.5 * local_params.astype(jnp.float32) + 0.5 * outer_new[None, :, :]).astype(jnp.bfloat16)
    return (keys, values, momentum_new, outer_new, local_new)
```

```python
import functools

import jax
import jax.numpy as jnp
from jax import lax
from jax.experimental import pallas as pl
from jax.experimental.pallas import tpu as pltpu
from jax.sharding import Mesh
from jax.sharding import PartitionSpec as P

HEAD = 128
KV = 1024
D = 4096
REPLICA = ("z_hi", "y", "core")
FSDP = ("x", "z")
AXES = REPLICA + FSDP
CHUNKS = ((0, 768), (768, 1536), (1536, 2048))


VMEM = pl.BlockSpec(memory_space=pltpu.VMEM)


def along_z(value, pairs):
    return lax.ppermute(value, "z", pairs)


def tokens_kernel(h_ref, out_ref, inv_ref, acc):
    step = pl.program_id(0)
    z = lax.axis_index("z")
    low = z < 2
    order = (z, z + 1 - 2 * (z % 2), jnp.where(low, 2, 1), jnp.where(low, 3, 0))

    @pl.when(step == 0)
    def _():
        acc[...] = jnp.zeros_like(acc)

    total = acc[...]
    for k in range(4):
        start = pl.multiple_of(order[k] * 256, 256)
        block = h_ref[:, pl.ds(start, 256)]
        out_ref[0, :, 256 * k : 256 * (k + 1)] = block
        wide = block.astype(jnp.float32)
        square = wide * wide
        total = total + square[:, :128] + square[:, 128:]
    acc[...] = total

    @pl.when(step == 3)
    def _():
        mean = jnp.sum(total, axis=1, keepdims=True) / D
        inv_ref[...] = jnp.broadcast_to(lax.rsqrt(mean + 1e-05), inv_ref.shape)


def spread_tokens(states):
    tokens = states.shape[0]
    return pl.pallas_call(
        tokens_kernel,
        grid=(4,),
        in_specs=[pl.BlockSpec((tokens, 1024), lambda i: (0, i))],
        out_specs=[
            pl.BlockSpec((1, tokens, 1024), lambda i: (i, 0, 0)),
            pl.BlockSpec((tokens, 128), lambda i: (0, 0)),
        ],
        out_shape=[
            jax.ShapeDtypeStruct((4, tokens, 1024), jnp.bfloat16),
            jax.ShapeDtypeStruct((tokens, 128), jnp.float32),
        ],
        scratch_shapes=[pltpu.VMEM((tokens, 128), jnp.float32)],
        name="spread_tokens",
    )(states)


def product_kernel(a_ref, w0, w1, w2m, w3m, w2e, w3e, out_ref):
    z = lax.axis_index("z")
    middle = (z == 1) | (z == 2)
    a = a_ref[0]
    dot = functools.partial(jnp.dot, preferred_element_type=jnp.float32)
    total = dot(a[:, 0:256], w0[...]) + dot(a[:, 256:512], w1[...])
    total += dot(a[:, 512:768], jnp.where(middle, w2m[...], w2e[...]))
    total += dot(a[:, 768:1024], jnp.where(middle, w3m[...], w3e[...]))
    out_ref[0] = total.astype(out_ref.dtype)


def product(rows, weights):
    blocks, tokens, _ = rows.shape
    width = weights[0].shape[1]
    return pl.pallas_call(
        product_kernel,
        grid=(blocks,),
        in_specs=[pl.BlockSpec((1, tokens, 1024), lambda i: (i, 0, 0))]
        + [pl.BlockSpec((256, width), lambda i: (0, 0))] * 6,
        out_specs=pl.BlockSpec((1, tokens, width), lambda i: (i, 0, 0)),
        out_shape=jax.ShapeDtypeStruct((blocks, tokens, width), jnp.bfloat16),
        name="product",
    )(rows, *weights)


def finish_kernel(n_keys, part_ref, inv_ref, cos_ref, sin_ref, *outs):
    inv = inv_ref[...]
    heads = part_ref.shape[2] // HEAD
    for h in range(heads):
        columns = slice(HEAD * h, HEAD * (h + 1))
        total = part_ref[0, :, columns].astype(jnp.float32)
        for k in range(1, 4):
            total = total + part_ref[k, :, columns].astype(jnp.float32)
        total = total * inv
        if h < n_keys:
            total = total * cos_ref[...] + pltpu.roll(total, HEAD // 2, 1) * sin_ref[...]
            outs[0][:, columns] = total.astype(jnp.bfloat16)
        else:
            outs[-1][:, HEAD * (h - n_keys) : HEAD * (h - n_keys + 1)] = total.astype(jnp.bfloat16)


def finish(parts, inv, cosine, sine, low, high):
    tokens = parts.shape[1]
    n_keys = max(0, min(high, KV) - low)
    widths = [w for w in (n_keys, high - low - n_keys) if w]
    out = pl.pallas_call(
        functools.partial(finish_kernel, n_keys // HEAD),
        in_specs=[VMEM] * 4,
        out_specs=[VMEM] * len(widths),
        out_shape=[jax.ShapeDtypeStruct((tokens, w), jnp.bfloat16) for w in widths],
        name="finish",
    )(parts, inv, cosine, sine)
    return (out[:1] if n_keys else []), (out[1 if n_keys else 0 :])


def split_deltas_kernel(d_ref, out_ref):
    for r in range(out_ref.shape[0]):
        out_ref[r] = d_ref[:, 128 * r : 128 * (r + 1)].astype(jnp.bfloat16)


def outer_kernel(d_ref, params_ref, momentum_ref, momentum_out, outer_out, spread_out):
    total = d_ref[0].astype(jnp.float32)
    for r in range(1, d_ref.shape[0]):
        total = total + d_ref[r].astype(jnp.float32)
    average = total / d_ref.shape[0]
    momentum_new = 0.9 * momentum_ref[...] + average
    outer_new = params_ref[...] - 0.7 * (average + 0.9 * momentum_new)
    momentum_out[...] = momentum_new
    outer_out[...] = outer_new
    for r in range(d_ref.shape[0]):
        spread_out[r] = outer_new


def merge_kernel(outer_ref, local_ref, out_ref):
    for r in range(outer_ref.shape[0]):
        columns = slice(128 * r, 128 * (r + 1))
        half = 0.5 * local_ref[:, columns].astype(jnp.float32)
        out_ref[:, columns] = (half + 0.5 * outer_ref[r]).astype(jnp.bfloat16)


def local_call(kernel, shapes, name):
    many = isinstance(shapes, list)
    return pl.pallas_call(
        kernel,
        out_specs=[VMEM] * len(shapes) if many else VMEM,
        out_shape=shapes,
        name=name,
    )


def turns(tokens):
    exponent = jnp.arange(HEAD // 2, dtype=jnp.float32) * (2.0 / HEAD)
    frequency = jnp.power(jnp.float32(500000.0), -exponent)
    angles = jnp.arange(tokens, dtype=jnp.int32).astype(jnp.float32)[:, None] * frequency[None, :]
    cosine, sine = jnp.cos(angles), jnp.sin(angles)
    return jnp.concatenate([cosine, cosine], axis=1), jnp.concatenate([-sine, sine], axis=1)


def per_device(
    hidden_states, norm_gain, key_weight, value_weight, deltas, outer_params, momentum, local_params
):
    shape, f32 = jax.ShapeDtypeStruct, jnp.float32
    states = hidden_states[0]
    tokens = states.shape[0]
    gain = norm_gain[0].astype(f32)[:, None]

    def own_rows(low, high):
        pieces = []
        if low < KV:
            pieces.append(key_weight[0, :, low : min(high, KV)])
        if high > KV:
            pieces.append(value_weight[0, :, max(low, KV) - KV : high - KV])
        rows = pieces[0] if len(pieces) == 1 else jnp.concatenate(pieces, axis=1)
        return (rows.astype(f32) * gain).astype(jnp.bfloat16)

    ends, middle, outward = [(0, 1), (1, 0), (2, 3), (3, 2)], [(1, 2), (2, 1)], [(1, 0), (2, 3)]
    gathered = []
    for low, high in CHUNKS:
        own = own_rows(low, high)
        mate = along_z(own, ends)
        third = along_z(own, middle)
        fourth = along_z(mate, middle)
        third_end = along_z(third, outward)
        fourth_end = along_z(fourth, outward)
        gathered.append((own, mate, third, fourth, third_end, fourth_end))

    spread, inv = spread_tokens(states)
    rows = lax.all_to_all(spread, "x", split_axis=0, concat_axis=0, tiled=True)

    n_replica = lax.axis_size(REPLICA)
    rows_f, columns_f = outer_params.shape
    split = local_call(
        split_deltas_kernel, shape((n_replica, rows_f, columns_f), jnp.bfloat16), "split_deltas"
    )(deltas[0])
    arrived = lax.all_to_all(split, REPLICA, split_axis=0, concat_axis=0, tiled=True)
    momentum_new, outer_new, outer_spread = local_call(
        outer_kernel,
        [shape((rows_f, columns_f), f32)] * 2 + [shape((n_replica, rows_f, columns_f), f32)],
        "outer_step",
    )(arrived, outer_params, momentum)
    outer_rows = lax.all_to_all(outer_spread, REPLICA, split_axis=0, concat_axis=0, tiled=True)
    local_new = local_call(
        merge_kernel, shape((rows_f, n_replica * columns_f), jnp.bfloat16), "merge"
    )(outer_rows, local_params[0])

    cosine, sine = turns(tokens)
    keys, values = [], []
    for (low, high), weights in zip(CHUNKS, gathered, strict=True):
        parts = product(rows, weights)
        parts = lax.all_to_all(parts, "x", split_axis=0, concat_axis=0, tiled=True)
        k, v = finish(parts, inv, cosine, sine, low, high)
        keys += k
        values += v
    keys = keys[0] if len(keys) == 1 else jnp.concatenate(keys, axis=1)
    values = values[0] if len(values) == 1 else jnp.concatenate(values, axis=1)
    return keys[None], values[None], momentum_new, outer_new, local_new[None]


def solution(mesh):
    split = Mesh(mesh.devices.reshape(2, 8, 2, 4, 4), AXES)
    return jax.shard_map(
        per_device,
        mesh=split,
        in_specs=(
            P(REPLICA, FSDP, None),
            P(REPLICA, FSDP),
            P(REPLICA, FSDP, None),
            P(REPLICA, FSDP, None),
            P(REPLICA, FSDP, None),
            P(FSDP, REPLICA),
            P(FSDP, REPLICA),
            P(REPLICA, FSDP, None),
        ),
        out_specs=(
            P(REPLICA, FSDP, None),
            P(REPLICA, FSDP, None),
            P(FSDP, REPLICA),
            P(FSDP, REPLICA),
            P(REPLICA, FSDP, None),
        ),
        check_vma=False,
    )
```

```python
import functools

import jax
import jax.numpy as jnp
from jax import lax
from jax.experimental import pallas as pl
from jax.experimental.pallas import tpu as pltpu
from jax.sharding import Mesh
from jax.sharding import PartitionSpec as P


HEAD = 128
KV = 1024
D = 4096
REPLICA = ("z_hi", "y", "core")
FSDP = ("x", "z")
AXES = REPLICA + FSDP
CHUNKS = ((0, 1280), (1280, 2048))
PARTS_AT_ONCE = (False, False)
TOKENS_AT_ONCE = False


VMEM = pl.BlockSpec(memory_space=pltpu.VMEM)
ANY = pl.BlockSpec(memory_space=pl.ANY)
PARAMS = pltpu.CompilerParams(vmem_limit_bytes=16 * 2**20)


def near(value):
    return pltpu.with_memory_space_constraint(value, pltpu.VMEM)


def along_z(value, pairs):
    return lax.ppermute(value, "z", pairs)


def along_x(value, shift):
    return lax.ppermute(value, "x", [(i, (i + shift) % 4) for i in range(4)])


def swapped(values, sign, at_once):
    if at_once:
        return [exchange(values[0], "x")]
    return [values[0]] + [along_x(values[r], sign * r) for r in (1, 2, 3)]


def exchange(value, axis):
    return lax.all_to_all(value, axis, split_axis=0, concat_axis=0, tiled=True)


def scale_kernel(gain_ref, *refs):
    rows = gain_ref.shape[1]
    same = lax.broadcasted_iota(jnp.int32, (rows, rows), 0) == lax.broadcasted_iota(
        jnp.int32, (rows, rows), 1
    )
    gain = jnp.where(same, gain_ref[...].astype(jnp.float32), 0.0)
    gain = jnp.sum(gain, axis=1, keepdims=True)
    out_ref, start = refs[-1], 0
    for ref in refs[:-1]:
        end = start + ref.shape[1]
        out_ref[:, start:end] = (ref[...].astype(jnp.float32) * gain).astype(jnp.bfloat16)
        start = end


def scaled_rows(gain, keys, values, low, high):
    rows = keys.shape[0]
    pieces, specs = [], []
    for array, first, last in (
        (keys, low, min(high, KV)),
        (values, max(low, KV) - KV, high - KV),
    ):
        for at in range(first, last, 256):
            pieces.append(array)
            specs.append(pl.BlockSpec((rows, 256), functools.partial(lambda c, i: (0, c), at // 256)))
    return pl.pallas_call(
        scale_kernel,
        grid=(1,),
        in_specs=[pl.BlockSpec((1, rows), lambda i: (0, 0))] + specs,
        out_specs=pl.BlockSpec((rows, high - low), lambda i: (0, 0)),
        out_shape=pltpu.VMEM((rows, high - low), jnp.bfloat16),
        compiler_params=PARAMS,
        name="scale",
    )(gain, *pieces)


def tokens_kernel(h_ref, *refs):
    outs, inv_ref = refs[:-1], refs[-1]
    x, z = lax.axis_index("x"), lax.axis_index("z")
    order = (z, z + 1 - 2 * (z % 2), (z + 2) % 4, 3 - z)
    total = jnp.zeros(inv_ref.shape, jnp.float32)
    for r in range(4):
        out_ref = outs[r] if len(outs) == 4 else outs[0].at[r]
        quarter = (x + r) % 4 if len(outs) == 4 else r
        for k in range(4):
            start = pl.multiple_of(quarter * 1024 + order[k] * 256, 256)
            block = h_ref[:, pl.ds(start, 256)]
            out_ref[:, 256 * k : 256 * (k + 1)] = block
            wide = block.astype(jnp.float32)
            square = wide * wide
            total = total + square[:, :128] + square[:, 128:]
    mean = jnp.sum(total, axis=1, keepdims=True) / D
    inv_ref[...] = jnp.broadcast_to(lax.rsqrt(mean + 1e-05), inv_ref.shape)


def spread_tokens(states):
    tokens = states.shape[0]
    if TOKENS_AT_ONCE:
        shapes = [pltpu.VMEM((4, tokens, 1024), jnp.bfloat16)]
    else:
        shapes = [pltpu.VMEM((tokens, 1024), jnp.bfloat16)] * 4
    return pl.pallas_call(
        tokens_kernel,
        in_specs=[VMEM],
        out_specs=[VMEM] * (len(shapes) + 1),
        out_shape=shapes + [pltpu.VMEM((tokens, 128), jnp.float32)],
        compiler_params=PARAMS,
        name="spread_tokens",
    )(states)


def product_kernel(n_rows, *refs):
    rows, pieces, refs = refs[:n_rows], refs[n_rows : n_rows + 4], refs[n_rows + 4 :]
    outs, (a_ref, w_ref) = refs[:-2], refs[-2:]
    x = lax.axis_index("x")
    tokens = outs[0].shape[-2]
    for k, piece in enumerate(pieces):
        w_ref[256 * k : 256 * (k + 1)] = piece[...]
    for r in range(4):
        a_ref[tokens * r : tokens * (r + 1)] = rows[r][...] if n_rows == 4 else rows[0][(x + 4 - r) % 4]
    for at in range(0, w_ref.shape[1], 256):
        columns = slice(at, at + 256)
        total = jnp.dot(a_ref[...], w_ref[:, columns], preferred_element_type=jnp.float32)
        for r in range(4):
            out = outs[r] if len(outs) == 4 else outs[0].at[(x + 4 - r) % 4]
            out[:, columns] = total[tokens * r : tokens * (r + 1)].astype(out.dtype)


def product(rows, weights, at_once):
    tokens, width = rows[0].shape[-2], weights[0].shape[1]
    shape = (tokens, width)
    if at_once:
        shapes = [pltpu.VMEM((4, *shape), jnp.bfloat16)]
    else:
        shapes = [pltpu.VMEM(shape, t) for t in (jnp.float32,) + (jnp.bfloat16,) * 3]
    return pl.pallas_call(
        functools.partial(product_kernel, len(rows)),
        in_specs=[VMEM] * (len(rows) + 4),
        out_specs=[VMEM] * len(shapes),
        out_shape=shapes,
        scratch_shapes=[
            pltpu.VMEM((4 * tokens, 1024), jnp.bfloat16),
            pltpu.VMEM((1024, width), jnp.bfloat16),
        ],
        compiler_params=PARAMS,
        name="product",
    )(*map(near, rows), *map(near, weights))


def finish_kernel(turned, skip, n_parts, *refs):
    parts, (inv_ref, cos_ref, sin_ref), out_ref = refs[:n_parts], refs[n_parts : n_parts + 3], refs[-1]
    blocks = parts if n_parts == 4 else [parts[0].at[r] for r in range(4)]
    inv = inv_ref[...]
    for h in range(out_ref.shape[1] // HEAD):
        at = pl.multiple_of(skip + pl.program_id(0) * out_ref.shape[1] + h * HEAD, HEAD)
        columns = pl.ds(at, HEAD)
        total = blocks[0][:, columns].astype(jnp.float32)
        for block in blocks[1:]:
            total = total + block[:, columns].astype(jnp.float32)
        total = total * inv
        if turned:
            total = total * cos_ref[...] + pltpu.roll(total, HEAD // 2, 1) * sin_ref[...]
        out_ref[:, HEAD * h : HEAD * (h + 1)] = total.astype(jnp.bfloat16)


def finish(parts, inv, cosine, sine, before, turned, skip, at, width):
    tokens = parts[0].shape[-2]
    have = [] if before is None else [before]
    return pl.pallas_call(
        functools.partial(finish_kernel, turned, skip, len(parts)),
        grid=(width // 256,),
        in_specs=[VMEM] * (len(parts) + 3) + [ANY] * len(have),
        out_specs=pl.BlockSpec((tokens, 256), lambda i: (0, at // 256 + i)),
        out_shape=jax.ShapeDtypeStruct((tokens, KV), jnp.bfloat16),
        input_output_aliases={len(parts) + 3: 0} if have else {},
        compiler_params=PARAMS,
        name="finish",
    )(*map(near, parts), *map(near, (inv, cosine, sine)), *have)


def split_deltas_kernel(d_ref, out_ref):
    for r in range(out_ref.shape[0]):
        out_ref[r] = d_ref[:, 128 * r : 128 * (r + 1)].astype(jnp.bfloat16)


def outer_kernel(d_ref, params_ref, momentum_ref, momentum_out, outer_out, spread_out):
    total = d_ref[0].astype(jnp.float32)
    for r in range(1, d_ref.shape[0]):
        total = total + d_ref[r].astype(jnp.float32)
    average = total / d_ref.shape[0]
    momentum_new = 0.9 * momentum_ref[...] + average
    outer_new = params_ref[...] - 0.7 * (average + 0.9 * momentum_new)
    momentum_out[...] = momentum_new
    outer_out[...] = outer_new
    for r in range(d_ref.shape[0]):
        spread_out[r] = outer_new


def merge_kernel(outer_ref, local_ref, out_ref):
    for r in range(outer_ref.shape[0]):
        columns = slice(128 * r, 128 * (r + 1))
        half = 0.5 * local_ref[:, columns].astype(jnp.float32)
        out_ref[:, columns] = (half + 0.5 * outer_ref[r]).astype(jnp.bfloat16)


def local_call(kernel, shapes):
    many = isinstance(shapes, list)
    return pl.pallas_call(
        kernel, out_specs=[VMEM] * len(shapes) if many else VMEM, out_shape=shapes, compiler_params=PARAMS
    )


def turns(tokens):
    exponent = jnp.arange(HEAD // 2, dtype=jnp.float32) * (2.0 / HEAD)
    frequency = jnp.power(jnp.float32(500000.0), -exponent)
    angles = jnp.arange(tokens, dtype=jnp.int32).astype(jnp.float32)[:, None] * frequency[None, :]
    cosine, sine = jnp.cos(angles), jnp.sin(angles)
    return jnp.concatenate([cosine, cosine], axis=1), jnp.concatenate([-sine, sine], axis=1)


def per_device(
    hidden_states, norm_gain, key_weight, value_weight, deltas, outer_params, momentum, local_params
):
    shape, f32 = jax.ShapeDtypeStruct, jnp.float32
    states = hidden_states[0]
    tokens = states.shape[0]
    first, second = [[(i, i ^ bit) for i in range(4)] for bit in (1, 2)]
    gathered = []
    for low, high in CHUNKS:
        own = scaled_rows(norm_gain, key_weight[0], value_weight[0], low, high)
        mate = along_z(own, first)
        two = along_z(own, second)
        gathered.append((own, mate, two, along_z(two, first)))

    *spread, inv = spread_tokens(states)
    rows = swapped(spread, 1, TOKENS_AT_ONCE)

    n_replica = lax.axis_size(REPLICA)
    rows_f, columns_f = outer_params.shape
    split = local_call(split_deltas_kernel, pltpu.VMEM((n_replica, rows_f, columns_f), jnp.bfloat16))(deltas[0])
    arrived = exchange(split, REPLICA)
    momentum_new, outer_new, outer_spread = local_call(
        outer_kernel, [shape((rows_f, columns_f), f32)] * 2 + [pltpu.VMEM((n_replica, rows_f, columns_f), f32)]
    )(near(arrived), outer_params, momentum)
    outer_rows = exchange(outer_spread, REPLICA)
    local_new = local_call(
        merge_kernel, shape((rows_f, n_replica * columns_f), jnp.bfloat16)
    )(near(outer_rows), local_params[0])

    cosine, sine = turns(tokens)
    keys = values = None
    for n, ((low, high), weights) in enumerate(zip(CHUNKS, gathered, strict=True)):
        parts = product(rows, weights, PARTS_AT_ONCE[n])
        parts = swapped(parts, -1, PARTS_AT_ONCE[n])
        if low < KV:
            width = min(high, KV) - low
            keys = finish(parts, inv, cosine, sine, keys, True, 0, low, width)
        if high > KV:
            at = max(low, KV) - KV
            skip = at + KV - low
            values = finish(parts, inv, cosine, sine, values, False, skip, at, high - KV - at)
    return keys[None], values[None], momentum_new, outer_new, local_new[None]


def solution(mesh):
    split = Mesh(mesh.devices.reshape(2, 8, 2, 4, 4), AXES)

    return jax.shard_map(
        per_device,
        mesh=split,
        in_specs=(
            P(REPLICA, FSDP, None),
            P(REPLICA, FSDP),
            P(REPLICA, FSDP, None),
            P(REPLICA, FSDP, None),
            P(REPLICA, FSDP, None),
            P(FSDP, REPLICA),
            P(FSDP, REPLICA),
            P(REPLICA, FSDP, None),
        ),
        out_specs=(
            P(REPLICA, FSDP, None),
            P(REPLICA, FSDP, None),
            P(FSDP, REPLICA),
            P(FSDP, REPLICA),
            P(REPLICA, FSDP, None),
        ),
        check_vma=False,
    )
```

```python
import functools

import jax
import jax.numpy as jnp
from jax import lax
from jax.experimental import pallas as pl
from jax.experimental.pallas import tpu as pltpu
from jax.sharding import Mesh
from jax.sharding import PartitionSpec as P


HEAD = 128
KV = 1024
D = 4096
REPLICA = ("z_hi", "y", "core")
FSDP = ("x", "z")
AXES = REPLICA + FSDP
CHUNKS = ((0, 1280), (1280, 2048))
PARTS_AT_ONCE = (False, False)
TOKENS_AT_ONCE = False


VMEM = pl.BlockSpec(memory_space=pltpu.VMEM)
ANY = pl.BlockSpec(memory_space=pl.ANY)
PARAMS = pltpu.CompilerParams(vmem_limit_bytes=16 * 2**20)


def near(value):
    return pltpu.with_memory_space_constraint(value, pltpu.VMEM)


def far(value):
    return pltpu.with_memory_space_constraint(value, pltpu.HBM)


def along_z(value, pairs):
    return lax.ppermute(value, "z", pairs)


def along_x(value, shift):
    return lax.ppermute(value, "x", [(i, (i + shift) % 4) for i in range(4)])


def swapped(values, sign, at_once):
    if at_once:
        return [exchange(values[0], "x")]
    return [values[0]] + [along_x(values[r], sign * r) for r in (1, 2, 3)]


def exchange(value, axis):
    return lax.all_to_all(value, axis, split_axis=0, concat_axis=0, tiled=True)


def scale_kernel(gain_ref, *refs):
    rows = gain_ref.shape[1]
    same = lax.broadcasted_iota(jnp.int32, (rows, rows), 0) == lax.broadcasted_iota(
        jnp.int32, (rows, rows), 1
    )
    gain = jnp.where(same, gain_ref[...].astype(jnp.float32), 0.0)
    gain = jnp.sum(gain, axis=1, keepdims=True)
    out_ref, start = refs[-1], 0
    for ref in refs[:-1]:
        end = start + ref.shape[1]
        out_ref[:, start:end] = (ref[...].astype(jnp.float32) * gain).astype(jnp.bfloat16)
        start = end


def scaled_rows(gain, keys, values, low, high):
    rows = keys.shape[0]
    pieces, specs = [], []
    for array, first, last in (
        (keys, low, min(high, KV)),
        (values, max(low, KV) - KV, high - KV),
    ):
        for at in range(first, last, 256):
            pieces.append(array)
            specs.append(pl.BlockSpec((rows, 256), functools.partial(lambda c, i: (0, c), at // 256)))
    return pl.pallas_call(
        scale_kernel,
        grid=(1,),
        in_specs=[pl.BlockSpec((1, rows), lambda i: (0, 0))] + specs,
        out_specs=pl.BlockSpec((rows, high - low), lambda i: (0, 0)),
        out_shape=pltpu.VMEM((rows, high - low), jnp.bfloat16),
        compiler_params=PARAMS,
        name="scale",
    )(far(gain), *map(far, pieces))


def tokens_kernel(h_ref, *refs):
    outs, inv_ref = refs[:-1], refs[-1]
    x, z = lax.axis_index("x"), lax.axis_index("z")
    order = (z, z + 1 - 2 * (z % 2), (z + 2) % 4, 3 - z)
    total = jnp.zeros(inv_ref.shape, jnp.float32)
    for r in range(4):
        out_ref = outs[r] if len(outs) == 4 else outs[0].at[r]
        quarter = (x + r) % 4 if len(outs) == 4 else r
        for k in range(4):
            start = pl.multiple_of(quarter * 1024 + order[k] * 256, 256)
            block = h_ref[:, pl.ds(start, 256)]
            out_ref[:, 256 * k : 256 * (k + 1)] = block
            wide = block.astype(jnp.float32)
            square = wide * wide
            total = total + square[:, :128] + square[:, 128:]
    mean = jnp.sum(total, axis=1, keepdims=True) / D
    inv_ref[...] = jnp.broadcast_to(lax.rsqrt(mean + 1e-05), inv_ref.shape)


def spread_tokens(states):
    tokens = states.shape[0]
    if TOKENS_AT_ONCE:
        shapes = [pltpu.VMEM((4, tokens, 1024), jnp.bfloat16)]
    else:
        shapes = [pltpu.VMEM((tokens, 1024), jnp.bfloat16)] * 4
    return pl.pallas_call(
        tokens_kernel,
        in_specs=[VMEM],
        out_specs=[VMEM] * (len(shapes) + 1),
        out_shape=shapes + [pltpu.VMEM((tokens, 128), jnp.float32)],
        compiler_params=PARAMS,
        name="spread_tokens",
    )(states)


def product_kernel(n_rows, *refs):
    rows, pieces, refs = refs[:n_rows], refs[n_rows : n_rows + 4], refs[n_rows + 4 :]
    outs, (a_ref, w_ref) = refs[:-2], refs[-2:]
    x = lax.axis_index("x")
    tokens = outs[0].shape[-2]
    for k, piece in enumerate(pieces):
        w_ref[256 * k : 256 * (k + 1)] = piece[...]
    for r in range(4):
        a_ref[tokens * r : tokens * (r + 1)] = rows[r][...] if n_rows == 4 else rows[0][(x + 4 - r) % 4]
    for at in range(0, w_ref.shape[1], 256):
        columns = slice(at, at + 256)
        total = jnp.dot(a_ref[...], w_ref[:, columns], preferred_element_type=jnp.float32)
        for r in range(4):
            out = outs[r] if len(outs) == 4 else outs[0].at[(x + 4 - r) % 4]
            out[:, columns] = total[tokens * r : tokens * (r + 1)].astype(out.dtype)


def product(rows, weights, at_once):
    tokens, width = rows[0].shape[-2], weights[0].shape[1]
    shape = (tokens, width)
    if at_once:
        shapes = [pltpu.VMEM((4, *shape), jnp.bfloat16)]
    else:
        shapes = [pltpu.HBM(shape, jnp.bfloat16)] + [pltpu.VMEM(shape, jnp.bfloat16)] * 3
    return pl.pallas_call(
        functools.partial(product_kernel, len(rows)),
        in_specs=[VMEM] * (len(rows) + 4),
        out_specs=[VMEM] * len(shapes),
        out_shape=shapes,
        scratch_shapes=[
            pltpu.VMEM((4 * tokens, 1024), jnp.bfloat16),
            pltpu.VMEM((1024, width), jnp.bfloat16),
        ],
        compiler_params=PARAMS,
        name="product",
    )(*map(near, rows), *map(near, weights))


def finish_kernel(turned, skip, n_parts, *refs):
    parts, (inv_ref, cos_ref, sin_ref), out_ref = refs[:n_parts], refs[n_parts : n_parts + 3], refs[-1]
    blocks = parts if n_parts == 4 else [parts[0].at[r] for r in range(4)]
    inv = inv_ref[...]
    for h in range(out_ref.shape[1] // HEAD):
        at = pl.multiple_of(skip + pl.program_id(0) * out_ref.shape[1] + h * HEAD, HEAD)
        columns = pl.ds(at, HEAD)
        total = blocks[0][:, columns].astype(jnp.float32)
        for block in blocks[1:]:
            total = total + block[:, columns].astype(jnp.float32)
        total = total * inv
        if turned:
            total = total * cos_ref[...] + pltpu.roll(total, HEAD // 2, 1) * sin_ref[...]
        out_ref[:, HEAD * h : HEAD * (h + 1)] = total.astype(jnp.bfloat16)


def finish(parts, inv, cosine, sine, before, turned, skip, at, width):
    tokens = parts[0].shape[-2]
    have = [] if before is None else [before]
    return pl.pallas_call(
        functools.partial(finish_kernel, turned, skip, len(parts)),
        grid=(width // 256,),
        in_specs=[VMEM] * (len(parts) + 3) + [ANY] * len(have),
        out_specs=pl.BlockSpec((tokens, 256), lambda i: (0, at // 256 + i)),
        out_shape=jax.ShapeDtypeStruct((tokens, KV), jnp.bfloat16),
        input_output_aliases={len(parts) + 3: 0} if have else {},
        compiler_params=PARAMS,
        name="finish",
    )(*parts[:-3], *map(near, (*parts[-3:], inv, cosine, sine)), *have)


def split_deltas_kernel(d_ref, out_ref):
    for r in range(out_ref.shape[0]):
        out_ref[r] = d_ref[:, 128 * r : 128 * (r + 1)].astype(jnp.bfloat16)


def outer_kernel(d_ref, params_ref, momentum_ref, momentum_out, outer_out, spread_out):
    total = d_ref[0].astype(jnp.float32)
    for r in range(1, d_ref.shape[0]):
        total = total + d_ref[r].astype(jnp.float32)
    average = total / d_ref.shape[0]
    momentum_new = 0.9 * momentum_ref[...] + average
    outer_new = params_ref[...] - 0.7 * (average + 0.9 * momentum_new)
    momentum_out[...] = momentum_new
    outer_out[...] = outer_new
    for r in range(d_ref.shape[0]):
        spread_out[r] = outer_new


def merge_kernel(outer_ref, local_ref, out_ref):
    for r in range(outer_ref.shape[0]):
        columns = slice(128 * r, 128 * (r + 1))
        half = 0.5 * local_ref[:, columns].astype(jnp.float32)
        out_ref[:, columns] = (half + 0.5 * outer_ref[r]).astype(jnp.bfloat16)


def local_call(kernel, shapes):
    many = isinstance(shapes, list)
    return pl.pallas_call(
        kernel, out_specs=[VMEM] * len(shapes) if many else VMEM, out_shape=shapes, compiler_params=PARAMS
    )


def turns(tokens):
    exponent = jnp.arange(HEAD // 2, dtype=jnp.float32) * (2.0 / HEAD)
    frequency = jnp.power(jnp.float32(500000.0), -exponent)
    angles = jnp.arange(tokens, dtype=jnp.int32).astype(jnp.float32)[:, None] * frequency[None, :]
    cosine, sine = jnp.cos(angles), jnp.sin(angles)
    return jnp.concatenate([cosine, cosine], axis=1), jnp.concatenate([-sine, sine], axis=1)


def per_device(
    hidden_states, norm_gain, key_weight, value_weight, deltas, outer_params, momentum, local_params
):
    shape, f32 = jax.ShapeDtypeStruct, jnp.float32
    states = hidden_states[0]
    tokens = states.shape[0]
    first, second = [[(i, i ^ bit) for i in range(4)] for bit in (1, 2)]
    gathered = []
    for low, high in CHUNKS:
        own = scaled_rows(norm_gain, key_weight[0], value_weight[0], low, high)
        mate = along_z(own, first)
        two = along_z(own, second)
        gathered.append((own, mate, two, along_z(two, first)))

    *spread, inv = spread_tokens(states)
    rows = swapped(spread, 1, TOKENS_AT_ONCE)

    n_replica = lax.axis_size(REPLICA)
    rows_f, columns_f = outer_params.shape
    split = local_call(split_deltas_kernel, pltpu.VMEM((n_replica, rows_f, columns_f), jnp.bfloat16))(deltas[0])
    arrived = exchange(split, REPLICA)
    momentum_new, outer_new, outer_spread = local_call(
        outer_kernel, [shape((rows_f, columns_f), f32)] * 2 + [pltpu.VMEM((n_replica, rows_f, columns_f), f32)]
    )(near(arrived), outer_params, momentum)
    outer_rows = exchange(outer_spread, REPLICA)
    local_new = local_call(
        merge_kernel, shape((rows_f, n_replica * columns_f), jnp.bfloat16)
    )(near(outer_rows), local_params[0])

    cosine, sine = turns(tokens)
    keys = values = None
    for n, ((low, high), weights) in enumerate(zip(CHUNKS, gathered, strict=True)):
        parts = product(rows, weights, PARTS_AT_ONCE[n])
        parts = swapped(parts, -1, PARTS_AT_ONCE[n])
        if low < KV:
            width = min(high, KV) - low
            keys = finish(parts, inv, cosine, sine, keys, True, 0, low, width)
        if high > KV:
            at = max(low, KV) - KV
            skip = at + KV - low
            values = finish(parts, inv, cosine, sine, values, False, skip, at, high - KV - at)
    return keys[None], values[None], momentum_new, outer_new, local_new[None]


def solution(mesh):
    split = Mesh(mesh.devices.reshape(2, 8, 2, 4, 4), AXES)

    return jax.shard_map(
        per_device,
        mesh=split,
        in_specs=(
            P(REPLICA, FSDP, None),
            P(REPLICA, FSDP),
            P(REPLICA, FSDP, None),
            P(REPLICA, FSDP, None),
            P(REPLICA, FSDP, None),
            P(FSDP, REPLICA),
            P(FSDP, REPLICA),
            P(REPLICA, FSDP, None),
        ),
        out_specs=(
            P(REPLICA, FSDP, None),
            P(REPLICA, FSDP, None),
            P(FSDP, REPLICA),
            P(FSDP, REPLICA),
            P(REPLICA, FSDP, None),
        ),
        check_vma=False,
    )
```
